512 devices in a mesh: rep: 32 (over z, y_hi), shard: 16 (over y_lo, x, core).
Axes of the slice: x: 4, y: 4 (y_hi: 2, y_lo: 2; y = y_hi * 2 + y_lo), z: 16, core: 2. Of those that a mesh axis runs over, the one named last changes fastest.
Arguments:
- memory: float32 [524288, 256], P(('rep', 'shard')), may hold values from -4 to 4
- anchor_rows: int32 [32, 3, 4096], P('rep', None, 'shard'), may hold values from 0 to 1023, as said below
- target_rows: int32 [32, 3, 4096], P('rep', None, 'shard'), may hold values from 0 to 1023, as said below
- event_times: int32 [32, 3, 4096], P('rep', None, 'shard'), may hold values from 0 to 4095
- block_ids: int32 [32, 3, 16], P(None, None, 'shard'), may hold values from 0 to 511
- frequency: float32 [100], replicated, may hold values from 0.001 to 0.3
- phase: float32 [100], replicated, may hold values from -3.140625 to 3.140625
- w_source: bfloat16 [256, 256], replicated, may hold values from -0.375 to 0.375
- w_other: bfloat16 [256, 256], replicated, may hold values from -0.375 to 0.375
- w_time: bfloat16 [100, 256], replicated, may hold values from -0.625 to 0.625
- b_message: float32 [256], replicated, may hold values from -3 to 3
- w_input: bfloat16 [256, 768], replicated, may hold values from -0.375 to 0.375
- w_hidden: bfloat16 [256, 768], replicated, may hold values from -0.375 to 0.375
- b_gates: float32 [768], replicated, may hold values from -3 to 3
Outputs:
- memory_out: float32 [524288, 256], P(('rep', 'shard'))
The draws below stay inside these ranges and needn't reach their ends.
Inputs may be any that keep to these rules, and one draw needn't show every extreme that they name: Position j names row j % 64 of the block of shard column j // 64 chosen by block_ids[g, b, j // 64]; in each group and batch, each position block j // 64 is named by exactly 512 of the 8192 entries of anchor_rows and target_rows together. `target_rows`: as for anchor_rows. `block_ids`: value q in shard column s names block q % 16 of the memory rows of the device with rep index q // 16 and shard index s; that device owns rows ((q // 16) * 16 + s) * 16 * 64 onwards, 1024 of them.
All inputs are finite; a program needn't handle non-finite values.
Results may differ from the reference program's by a relative error of at most 0.00093.
Values may be sent and summed in bfloat16 or wider, within the bound.
A program may use at most 64 MiB of HBM per device.

```python
import math
import jax
import jax.numpy as jnp
from jax import lax

MEM = 256
MSG = 256
TD = 100
BLK = 64
EV_DEV = 256
BLK_DEV = 16
BATCHES = 3
SHARDS = 16
GROUPS = 32
TROWS = 1024
EVENTS = 4096
NODES = 524288
N_REP = 32
N_SHARD = 16


def endpoint_pairs(key):
    folded = jax.random.fold_in(key, 4711)
    first_key, second_key = jax.random.split(folded)
    shape = (GROUPS, BATCHES, 2 * EVENTS)
    starts = jnp.arange(2 * EVENTS, dtype=jnp.int32) // (2 * EV_DEV) * BLK
    base = jnp.broadcast_to(starts, shape)
    mixed = jax.random.permutation(first_key, base, axis=2, independent=True)
    within = jax.random.randint(second_key, shape, 0, BLK, dtype=jnp.int32)
    joined = (mixed + within).astype(jnp.int32)
    return (joined[:, :, :EVENTS], joined[:, :, EVENTS:])


def draw_anchor_rows(key, part):
    return endpoint_pairs(key)[0]


def draw_target_rows(key, part):
    return endpoint_pairs(key)[1]


def place_ends(result, key, low, largest):
    longest = result.shape.index(max(result.shape))
    spots = []
    for shift in (0, 1):
        where = [jax.random.randint(jax.random.fold_in(key, axis), (), 0, length) for axis, length in enumerate(result.shape)]
        where[longest] = (where[longest] + shift) % result.shape[longest]
        spots.append(tuple(where))
    return result.at[spots[0]].set(low).at[spots[1]].set(largest)


def steps_of(own_key, extent, cuts, least, high):
    def one(dim, shards_of):
        draws = jax.random.uniform(jax.random.fold_in(jax.random.fold_in(own_key, 6), dim), (shards_of,), jnp.float32, least / len(cuts), high / len(cuts))
        return jnp.repeat(jnp.exp(draws), extent[dim] // shards_of).reshape((-1,) + (1,) * (len(extent) - dim - 1))

    factor_of = one(*cuts[0])
    for cut in cuts[1:]:
        factor_of = factor_of * one(*cut)
    return factor_of


def noise(stream_key, shape, scale, reach, shards=(), kind=jnp.bfloat16):
    drawn = jax.random.normal(stream_key, shape, jnp.float32) * scale
    if len(shards) > 0:
        drawn = steps_of(stream_key, shape, shards, -0.22, 0.18) * drawn
    return jnp.clip(drawn, min=-reach, max=reach).astype(kind)


def setup_inputs(seed: int = 0) -> dict:
    seeds = jax.random.split(jax.random.key(seed), 15)
    return {
        "memory": noise(seeds[0], (NODES, MEM), 1.0, 4.0, ((0, 512),), jnp.float32),
        "anchor_rows": draw_anchor_rows(jax.random.fold_in(seeds[14], 71), 0),
        "target_rows": draw_target_rows(jax.random.fold_in(seeds[14], 71), 0),
        "event_times": place_ends(jax.random.randint(seeds[3], (GROUPS, BATCHES, EVENTS), 0, EVENTS), jax.random.fold_in(seeds[3], 1), 0, EVENTS - 1).astype(jnp.int32),
        "block_ids": place_ends(jax.random.randint(seeds[4], (GROUPS, BATCHES, SHARDS), 0, GROUPS * BLK_DEV), jax.random.fold_in(seeds[4], 1), 0, (GROUPS * BLK_DEV) - 1).astype(jnp.int32),
        "frequency": jnp.clip(jnp.exp(jax.random.uniform(seeds[5], (TD,), jnp.float32, math.log(0.001), math.log(0.3))), 0.001, 0.3),
        "phase": jnp.clip(jax.random.uniform(seeds[6], (TD,), jnp.float32, -3.140625, 3.140625), -3.140625, 3.140625),
        "w_source": noise(seeds[7], (MEM, MSG), MEM ** -0.5, 0.375),
        "w_other": noise(seeds[8], (MEM, MSG), MEM ** -0.5, 0.375),
        "w_time": noise(seeds[9], (TD, MSG), TD ** -0.5, 0.625),
        "b_message": noise(seeds[10], (MSG,), 0.5, 3.0, (), jnp.float32),
        "w_input": noise(seeds[11], (MSG, 3 * MEM), MSG ** -0.5, 0.375),
        "w_hidden": noise(seeds[12], (MEM, 3 * MEM), MEM ** -0.5, 0.375),
        "b_gates": noise(seeds[13], (3 * MEM,), 0.5, 3.0, (), jnp.float32),
    }


def gated_delta(state, message, w_input, w_hidden, b_gates):
    inputs = jnp.dot(message, w_input, preferred_element_type=jnp.float32)
    hidden = jnp.dot(state, w_hidden, preferred_element_type=jnp.float32)
    reset = jax.nn.sigmoid(inputs[:, :MEM] + hidden[:, :MEM] + b_gates[:MEM])
    update = jax.nn.sigmoid(inputs[:, MEM:2 * MEM] + hidden[:, MEM:2 * MEM] + b_gates[MEM:2 * MEM])
    candidate = jnp.tanh(inputs[:, 2 * MEM:] + b_gates[2 * MEM:] + reset * hidden[:, 2 * MEM:])
    return ((1.0 - update) * (candidate - state.astype(jnp.float32))).astype(jnp.bfloat16)


def reference(memory, anchor_rows, target_rows, event_times, block_ids, frequency, phase, w_source, w_other, w_time, b_message, w_input, w_hidden, b_gates):
    positions = jnp.arange(TROWS, dtype=jnp.int32)
    mem = memory
    for batch_index in range(BATCHES):
        def one_group(replica):
            blocks = block_ids[replica, batch_index][positions // BLK]
            nodes = (((blocks // BLK_DEV) * N_SHARD + positions // BLK) * (BLK_DEV * BLK) + (blocks % BLK_DEV) * BLK + positions % BLK).astype(jnp.int32)
            touched = mem[nodes].astype(jnp.bfloat16)
            anchor = anchor_rows[replica, batch_index]
            target = target_rows[replica, batch_index]
            events = anchor.shape[0]
            rows = jnp.concatenate([anchor, target]).astype(jnp.int32)
            state = touched[rows]
            encoding = jnp.cos(event_times[replica, batch_index].astype(jnp.float32)[:, None] * frequency[None, :] + phase[None, :]).astype(jnp.bfloat16)
            timed = jnp.dot(encoding, w_time, preferred_element_type=jnp.float32) + b_message
            own_part = jnp.dot(state, w_source, preferred_element_type=jnp.float32)
            other_part = jnp.dot(state, w_other, preferred_element_type=jnp.float32)
            upper = own_part[:events] + other_part[events:] + timed
            lower = own_part[events:] + other_part[:events] + timed
            message = jax.nn.relu(jnp.concatenate([upper, lower])).astype(jnp.bfloat16)
            delta = gated_delta(state, message, w_input, w_hidden, b_gates)
            group_delta = jnp.zeros((TROWS, MEM), jnp.float32).at[rows].add(delta.astype(jnp.float32))
            group_count = jnp.zeros((TROWS,), jnp.float32).at[rows].add(1.0)
            return nodes, group_delta, group_count

        nodes, group_delta, group_count = lax.map(one_group, jnp.arange(N_REP, dtype=jnp.int32))
        flat_nodes = nodes.reshape(-1)
        count = jnp.zeros((NODES,), jnp.float32).at[flat_nodes].add(group_count.reshape(-1))
        scale = 1.0 / jnp.maximum(count[flat_nodes], 1.0)
        mem = mem.at[flat_nodes].add(group_delta.reshape(-1, MEM) * scale[:, None])
    return mem
```

```python
import functools

import jax
import jax.numpy as jnp
from jax import lax
from jax.experimental import pallas as pl
from jax.experimental.pallas import tpu as pltpu
from jax.sharding import PartitionSpec as P

BLK = 64
BATCHES = 3
CNT = 8
MESH = pl.DeviceIdType.MESH
VM = pl.BlockSpec(memory_space=pltpu.VMEM)
SM = pl.BlockSpec(memory_space=pltpu.SMEM)


def copy_for_each(x, axis):
    copies = jnp.broadcast_to(x, (lax.axis_size(axis), *x.shape))
    return lax.all_to_all(copies, axis, split_axis=0, concat_axis=0, tiled=True)


def place(n_z):
    me = lax.axis_index("rep")
    z = me // 2
    y = me - 2 * z
    up = lax.rem(z + 1, n_z) * 2 + y
    down = lax.rem(z + n_z - 1, n_z) * 2 + y
    partner = 2 * z + 1 - y
    return me, z, y, up, down, partner


def greet(reps, shards):
    barrier = pltpu.get_barrier_semaphore()
    for other in reps:
        pl.semaphore_signal(barrier, inc=1, device_id={"rep": other}, device_id_type=MESH)
    for other in shards:
        pl.semaphore_signal(barrier, inc=1, device_id={"shard": other}, device_id_type=MESH)
    pl.semaphore_wait(barrier, len(reps) + len(shards))


def send(src, dst, send_sem, recv_sem, to, axis="rep"):
    return pltpu.make_async_remote_copy(
        src_ref=src, dst_ref=dst, send_sem=send_sem, recv_sem=recv_sem, device_id={axis: to}, device_id_type=MESH
    )


def stage_kernel(me_ref, owner_ref, slot_ref, mem_ref, match_ref, cnt_ref, out_ref, cnt_out_ref):
    me = me_ref[0]
    groups = out_ref.shape[0]

    def one(i, carry):
        group = i // BATCHES
        b = i - group * BATCHES
        mine = owner_ref[i] == me

        @pl.when(mine)
        def _():
            out_ref[group, b] = mem_ref[pl.ds(pl.multiple_of(slot_ref[i] * BLK, BLK), BLK), :].astype(jnp.bfloat16)

        @pl.when(jnp.logical_not(mine))
        def _():
            out_ref[group, b] = jnp.zeros(out_ref.shape[2:], jnp.bfloat16)

        return carry

    lax.fori_loop(0, groups * BATCHES, one, 0)
    for group in range(groups):
        cnt_out_ref[group] = cnt_ref[...] * match_ref[group]


def stage(me, owner, slot, mem, match, cnt):
    groups, width = match.shape[0], mem.shape[1]
    return pl.pallas_call(
        stage_kernel,
        out_shape=(jax.ShapeDtypeStruct((groups, BATCHES, BLK, width), jnp.bfloat16),
                   jax.ShapeDtypeStruct((groups, 8, 128), jnp.float32)),
        in_specs=[SM, SM, SM, VM, VM, VM],
        out_specs=(VM, VM),
        compiler_params=pltpu.CompilerParams(vmem_limit_bytes=32 << 20),
        name="stage",
    )(me, owner, slot, mem, match, cnt)


def fetch_kernel(n_z, stage_ref, cnt_ref, out_ref, tot_ref, up_out, up_in, down_out, down_in, y_out, y_in,
                 up_cout, up_cin, down_cout, down_cin, yc_out, yc_in, y_send, y_recv, z_send, z_recv):
    me, z, y, up, down, partner = place(n_z)
    half = n_z // 2
    greet((up, down, partner), ())
    ways = ((0, up, up_out, up_in, up_cout, up_cin, half), (1, down, down_out, down_in, down_cout, down_cin, half - 1))
    sent = []

    def block_copy(lane, step, b, j):
        way, to, outs, ins = lane[:4]
        return send(outs.at[step, b, j], ins.at[step, b, j], z_send.at[way, step, 2 * b + j], z_recv.at[way, step, 2 * b + j], to)

    def count_copy(lane, step):
        way, to, outs, ins = lane[0], lane[1], lane[4], lane[5]
        return send(outs.at[step], ins.at[step], z_send.at[way, step, 2 * BATCHES], z_recv.at[way, step, 2 * BATCHES], to)

    def towards(way, ahead):
        return lax.rem(z + (ahead if way == 0 else n_z - ahead), n_z) * 2

    for step in range(half):
        for b in range(BATCHES):
            for j in (0, 1):
                for lane in ways:
                    way, to, outs, ins = lane[:4]
                    if step >= lane[6]:
                        continue
                    mine = stage_ref[towards(way, lane[6] - step) + j, b]
                    if step > 0:
                        block_copy(lane, step - 1, b, j).wait_recv()
                        mine = mine + ins[step - 1, b, j]
                    outs[step, b, j] = mine
                    copy = block_copy(lane, step, b, j)
                    copy.start()
                    sent.append(copy)
        for lane in ways:
            if step >= lane[6]:
                continue
            dest = towards(lane[0], lane[6] - step)
            if step > 0:
                count_copy(lane, step - 1).wait_recv()
            for j in (0, 1):
                mine = cnt_ref[dest + j]
                lane[4][step, j] = mine if step == 0 else mine + lane[5][step - 1, j]
            copy = count_copy(lane, step)
            copy.start()
            sent.append(copy)
    here = 2 * z
    last = []
    for b in range(BATCHES):
        sums = []
        for j in (0, 1):
            for lane in ways:
                block_copy(lane, lane[6] - 1, b, j).wait_recv()
            sums.append(stage_ref[here + j, b] + (up_in[half - 1, b, j] + down_in[half - 2, b, j]))
        y_out[b] = jnp.where(y == 0, sums[1], sums[0])
        out_ref[b] = jnp.where(y == 0, sums[0], sums[1])
        copy = send(y_out.at[b], y_in.at[b], y_send.at[b], y_recv.at[b], partner)
        copy.start()
        last.append(copy)
    for lane in ways:
        count_copy(lane, lane[6] - 1).wait_recv()
    sums = [cnt_ref[here + j] + (up_cin[half - 1, j] + down_cin[half - 2, j]) for j in (0, 1)]
    yc_out[...] = jnp.where(y == 0, sums[1], sums[0])
    copy = send(yc_out, yc_in, y_send.at[BATCHES], y_recv.at[BATCHES], partner)
    copy.start()
    for b in range(BATCHES):
        last[b].wait_recv()
        out_ref[b] = out_ref[b] + y_in[b]
    copy.wait_recv()
    tot_ref[...] = jnp.where(y == 0, sums[0], sums[1]) + yc_in[...]
    for done in last + [copy] + sent:
        done.wait_send()


def fetch(staged, counts):
    n_rep, _, _, width = staged.shape
    half = n_rep // 4
    buf = pltpu.VMEM((half, BATCHES, 2, BLK, width), jnp.bfloat16)
    one = pltpu.VMEM((BATCHES, BLK, width), jnp.bfloat16)
    cbuf = pltpu.VMEM((half, 2, 8, 128), jnp.float32)
    cone = pltpu.VMEM((8, 128), jnp.float32)
    n_sem = 2 * BATCHES + 1
    return pl.pallas_call(
        functools.partial(fetch_kernel, n_rep // 2),
        out_shape=(jax.ShapeDtypeStruct((BATCHES, BLK, width), jnp.bfloat16), jax.ShapeDtypeStruct((8, 128), jnp.float32)),
        in_specs=[VM, VM],
        out_specs=(VM, VM),
        scratch_shapes=[
            buf, buf, buf, buf, one, one, cbuf, cbuf, cbuf, cbuf, cone, cone,
            pltpu.SemaphoreType.DMA((BATCHES + 1,)), pltpu.SemaphoreType.DMA((BATCHES + 1,)),
            pltpu.SemaphoreType.DMA((2, half, n_sem)), pltpu.SemaphoreType.DMA((2, half, n_sem)),
        ],
        compiler_params=pltpu.CompilerParams(collective_id=2, has_side_effects=True, vmem_limit_bytes=32 << 20),
        name="fetch",
    )(staged, counts)


def steps_kernel(n_z, n_shard, init_ref, meta_ref, timed_ref, tot_ref, match_ref, ws_ref, wo_ref, wi_ref, wh_ref, bg_ref,
                 all_ref, touched_ref, block_ref, pay_ref, y_send, y_recv, z_send, z_recv, s_send, s_recv):
    me, z, y, up, down, partner = place(n_z)
    shard = lax.axis_index("shard")
    half = n_z // 2
    width = init_ref.shape[2]
    ends = meta_ref.shape[1]
    rows = touched_ref.shape[1]
    peers = [lax.rem(shard + i, n_shard) for i in range(1, n_shard)]
    greet((up, down, partner), peers)
    my_rows = pl.ds(pl.multiple_of(shard * BLK, BLK), BLK)
    bias = bg_ref[...]
    eye = lax.broadcasted_iota(jnp.int32, (BLK, 128), 0) == lax.broadcasted_iota(jnp.int32, (BLK, 128), 1)

    for b in range(BATCHES):
        acc = init_ref[b].astype(jnp.float32)
        for earlier in range(b):
            pair = earlier if b == 1 else 1 + earlier

            def add(group, total, earlier=earlier, pair=pair):
                return total + match_ref[pair, pl.ds(group, 1), :] * all_ref[earlier, group].astype(jnp.float32)

            acc = lax.fori_loop(0, 2 * n_z, add, acc)
        block = acc.astype(jnp.bfloat16)
        block_ref[b] = block
        touched_ref[b, my_rows, :] = block
        out_copies = []
        for i, peer in enumerate(peers):
            copy = send(block_ref.at[b], touched_ref.at[b, my_rows, :], s_send.at[b, i], s_recv.at[b, i], peer, "shard")
            copy.start()
            out_copies.append(copy)
        meta = meta_ref[b]
        own_pick = jnp.where(lax.broadcasted_iota(jnp.int32, (ends, BLK), 1).astype(jnp.float32) == meta[:, 0:1], 1.0, 0.0).astype(jnp.bfloat16)
        own = jnp.dot(own_pick, block, preferred_element_type=jnp.float32)
        own16 = own.astype(jnp.bfloat16)
        gh = jnp.dot(own16, wh_ref[...], preferred_element_type=jnp.float32)
        message = jnp.dot(own16, ws_ref[...], preferred_element_type=jnp.float32) + timed_ref[b]
        other_at = meta[:, 1:2] * float(BLK) + meta[:, 2:3]
        other_pick = jnp.where(lax.broadcasted_iota(jnp.int32, (ends, rows), 1).astype(jnp.float32) == other_at, 1.0, 0.0).astype(jnp.bfloat16)
        for i in range(n_shard - 1):
            theirs = touched_ref.at[b, pl.ds(pl.multiple_of(lax.rem(shard + n_shard - 1 - i, n_shard) * BLK, BLK), BLK), :]
            send(theirs, theirs, s_send.at[b, i], s_recv.at[b, i], peers[i], "shard").wait_recv()
        other = jnp.dot(other_pick, touched_ref[b], preferred_element_type=jnp.float32).astype(jnp.bfloat16)
        message = message + jnp.dot(other, wo_ref[...], preferred_element_type=jnp.float32)
        message = jnp.maximum(message, 0.0).astype(jnp.bfloat16)
        gi = jnp.dot(message, wi_ref[...], preferred_element_type=jnp.float32)
        reset = jax.nn.sigmoid(gi[:, :width] + gh[:, :width] + bias[:, :width])
        update = jax.nn.sigmoid(gi[:, width : 2 * width] + gh[:, width : 2 * width] + bias[:, width : 2 * width])
        candidate = jnp.tanh(gi[:, 2 * width :] + bias[:, 2 * width :] + reset * gh[:, 2 * width :])
        delta = ((1.0 - update) * (candidate - own)).astype(jnp.bfloat16)
        group_delta = lax.dot_general(own_pick, delta, (((0,), (0,)), ((), ())), preferred_element_type=jnp.float32)
        count = jnp.sum(jnp.where(eye, tot_ref[b : b + 1, :], 0.0), axis=1, keepdims=True)
        payload = (group_delta * (1.0 / jnp.maximum(count, 1.0))).astype(jnp.bfloat16)
        pay_ref[b] = payload
        all_ref[b, me] = payload

        def origin_of(way, stream, back, n_z=n_z):
            return lax.rem(z + (n_z - back if way == 0 else back), n_z) * 2 + (y if stream == 0 else 1 - y)

        def hop(way, stream, step, b=b):
            origin = origin_of(way, stream, step - 1)
            dst = all_ref.at[b, origin]
            src = pay_ref.at[b] if (step == 1 and stream == 0) else dst
            return send(src, dst, z_send.at[b, way, stream, step - 1], z_recv.at[b, way, stream, step - 1], up if way == 0 else down)

        def arrival(way, stream, step, b=b):
            ref = all_ref.at[b, origin_of(way, stream, step)]
            return send(ref, ref, z_send.at[b, way, stream, step - 1], z_recv.at[b, way, stream, step - 1], up if way == 0 else down)

        across = send(pay_ref.at[b], all_ref.at[b, me], y_send.at[b], y_recv.at[b], partner)
        across.start()
        out_copies.append(across)

        def go(way, stream, step):
            copy = hop(way, stream, step)
            copy.start()
            out_copies.append(copy)

        go(0, 0, 1)
        go(1, 0, 1)
        theirs = all_ref.at[b, partner]
        send(theirs, theirs, y_send.at[b], y_recv.at[b], partner).wait_recv()
        go(0, 1, 1)
        go(1, 1, 1)
        for step in range(1, half + 1):
            for stream in (0, 1):
                for way in (0, 1):
                    steps = half if way == stream else half - 1
                    if step <= steps:
                        arrival(way, stream, step).wait_recv()
                        if step < steps:
                            go(way, stream, step + 1)
        for copy in out_copies:
            copy.wait_send()


def run_steps(init, meta, timed, tot, match, ws, wo, wi, wh, bg, n_rep, n_shard):
    width = init.shape[2]
    n_z = n_rep // 2
    block = pltpu.VMEM((BATCHES, BLK, width), jnp.bfloat16)
    ring = pltpu.SemaphoreType.DMA((BATCHES, 2, 2, n_z // 2))
    across = pltpu.SemaphoreType.DMA((BATCHES,))
    peers = pltpu.SemaphoreType.DMA((BATCHES, n_shard - 1))
    return pl.pallas_call(
        functools.partial(steps_kernel, n_z, n_shard),
        out_shape=jax.ShapeDtypeStruct((BATCHES, n_rep, BLK, width), jnp.bfloat16),
        in_specs=[VM] * 10,
        out_specs=VM,
        scratch_shapes=[pltpu.VMEM((BATCHES, n_shard * BLK, width), jnp.bfloat16), block, block,
                        across, across, ring, ring, peers, peers],
        compiler_params=pltpu.CompilerParams(collective_id=1, has_side_effects=True, vmem_limit_bytes=56 << 20),
        name="steps",
    )(init, meta, timed, tot, match, ws, wo, wi, wh, bg)


def update_kernel(me_ref, owner_ref, slot_ref, all_ref, mem_ref, out_ref):
    groups = all_ref.shape[1]
    me = me_ref[0]
    out_ref[...] = mem_ref[...]
    for b in range(BATCHES):

        def add(group, carry, b=b):
            i = group * BATCHES + b

            @pl.when(owner_ref[i] == me)
            def _():
                rows = pl.ds(pl.multiple_of(slot_ref[i] * BLK, BLK), BLK)
                out_ref[rows, :] += all_ref[b, group].astype(jnp.float32)

            return carry

        lax.fori_loop(0, groups, add, 0)


def update(me, owner, slot, gathered, mem):
    return pl.pallas_call(
        update_kernel,
        out_shape=jax.ShapeDtypeStruct(mem.shape, mem.dtype),
        in_specs=[SM, SM, SM, VM, VM],
        out_specs=VM,
        compiler_params=pltpu.CompilerParams(vmem_limit_bytes=32 << 20),
        name="update",
    )(me, owner, slot, gathered, mem)


def local(memory, anchor_rows, target_rows, event_times, block_ids, frequency, phase, w_source, w_other, w_time,
          b_message, w_input, w_hidden, b_gates):
    width = memory.shape[1]
    block_count = memory.shape[0] // BLK
    n_rep, n_shard = lax.axis_size("rep"), lax.axis_size("shard")
    replica = lax.axis_index("rep")
    me = replica.astype(jnp.int32).reshape(1)
    shard = lax.axis_index("shard").astype(jnp.int32).reshape(1)
    events = jnp.stack([anchor_rows[0], target_rows[0], event_times[0]], axis=1).reshape(3 * BATCHES, -1)
    events = jnp.moveaxis(copy_for_each(events[None], "shard").reshape(-1, *events.shape), 0, 1)
    meta, cnt = compact(shard, events, width)
    ids = block_ids[:, :, 0]
    own_ids = lax.dynamic_index_in_dim(ids, replica, 0, keepdims=False)
    owner, slot = (ids // block_count).reshape(-1), (ids % block_count).reshape(-1)
    same = jnp.pad((ids == own_ids[None, :]).astype(jnp.float32), ((0, 0), (0, 8 - BATCHES)))
    staged, counts = stage(me, owner, slot, memory, jnp.broadcast_to(same[:, :, None], (*same.shape, 128)),
                           jnp.pad(cnt[:, 0, :128], ((0, 8 - BATCHES), (0, 0))))
    init, total = fetch(staged, counts)
    when = meta[:, :, 3:4] * float(BLK) + meta[:, :, 4:5]
    encoding = jnp.cos(when * frequency + phase).astype(jnp.bfloat16)
    timed = jnp.dot(encoding, w_time, preferred_element_type=jnp.float32) + b_message
    pairs = [(0, 1), (0, 2), (1, 2)]
    match = jnp.stack([(ids[:, e] == own_ids[t]).astype(jnp.float32) for e, t in pairs])
    match = jnp.broadcast_to(match[:, :, None], (*match.shape, width))
    gathered = run_steps(init, meta, timed, total, match, w_source, w_other, w_input, w_hidden, b_gates.reshape(1, -1), n_rep, n_shard)
    return update(me, owner, slot, gathered, memory)


def compact_kernel(shard_ref, ev_ref, out_ref, cnt_ref):
    shard = shard_ref[0]
    sources, events = ev_ref.shape[1], ev_ref.shape[2]
    wide = 2 * events
    before = lax.broadcasted_iota(jnp.int32, (wide, wide), 0)
    after = lax.broadcasted_iota(jnp.int32, (wide, wide), 1)
    upto = jnp.where(before <= after, 1.0, 0.0).astype(jnp.bfloat16)
    rows16 = lax.broadcasted_iota(jnp.int32, (sources, sources), 0)
    cols16 = lax.broadcasted_iota(jnp.int32, (sources, sources), 1)
    lower = jnp.where(cols16 < rows16, 1.0, 0.0).astype(jnp.bfloat16)
    place_of = lax.broadcasted_iota(jnp.int32, (wide, wide), 0).astype(jnp.float32)
    field = lax.broadcasted_iota(jnp.int32, (8, wide), 0)
    local = lax.broadcasted_iota(jnp.int32, (BLK, wide), 0).astype(jnp.float32)
    for b in range(BATCHES):
        anchor, target, when = ev_ref[3 * b], ev_ref[3 * b + 1], ev_ref[3 * b + 2]
        own = jnp.concatenate([anchor, target], axis=1)
        other = jnp.concatenate([target, anchor], axis=1)
        when = jnp.concatenate([when, when], axis=1)
        mine = (own // BLK) == shard
        mask = jnp.where(mine, 1.0, 0.0).astype(jnp.bfloat16)
        rank = jnp.dot(mask, upto, preferred_element_type=jnp.float32)
        earlier = jnp.dot(lower, mask, preferred_element_type=jnp.float32)
        start = jnp.sum(earlier, axis=1, keepdims=True)
        dest = jnp.where(mine, start + rank - 1.0, -1.0)
        total = jnp.zeros((wide, 8), jnp.float32)
        count = jnp.zeros((BLK, 1), jnp.float32)
        for k in range(sources):
            o, p, t = own[k : k + 1], other[k : k + 1], when[k : k + 1]
            vals = jnp.where(field == 0, o % BLK,
                   jnp.where(field == 1, p // BLK,
                   jnp.where(field == 2, p % BLK,
                   jnp.where(field == 3, t // BLK,
                   jnp.where(field == 4, t % BLK, 0))))).astype(jnp.float32).astype(jnp.bfloat16)
            pick = jnp.where(place_of == dest[k : k + 1], 1.0, 0.0).astype(jnp.bfloat16)
            total += lax.dot_general(pick, vals, (((1,), (1,)), ((), ())), preferred_element_type=jnp.float32)
            here = jnp.where(mine[k : k + 1], (o % BLK).astype(jnp.float32), -1.0)
            count += jnp.sum(jnp.where(local == here, 1.0, 0.0), axis=1, keepdims=True)
        out_ref[b] = total
        eye = lax.broadcasted_iota(jnp.int32, (BLK, 128), 0) == lax.broadcasted_iota(jnp.int32, (BLK, 128), 1)
        row = jnp.sum(jnp.where(eye, count, 0.0), axis=0, keepdims=True)
        cnt_ref[b] = jnp.broadcast_to(jnp.concatenate([row, row], axis=1), cnt_ref.shape[1:])


def compact(shard, events, width):
    wide = 2 * events.shape[2]
    return pl.pallas_call(
        compact_kernel,
        out_shape=(jax.ShapeDtypeStruct((BATCHES, wide, 8), jnp.float32),
                   jax.ShapeDtypeStruct((BATCHES, CNT, width), jnp.float32)),
        in_specs=[SM, VM],
        out_specs=(VM, VM),
        compiler_params=pltpu.CompilerParams(vmem_limit_bytes=48 << 20),
        name="compact",
    )(shard, events)


def solution(mesh):
    in_specs = (P(("rep", "shard"), None), P("rep", None, "shard"), P("rep", None, "shard"), P("rep", None, "shard"),
                P(None, None, "shard")) + (P(),) * 9
    return jax.shard_map(local, mesh=mesh, in_specs=in_specs, out_specs=P(("rep", "shard"), None), check_vma=False)
```
